32 devices in a mesh: expert: 2 (over x), dp: 16 (over z, y, core).
Axes of the slice: x: 2, y: 2, z: 4, core: 2. Of those that a mesh axis runs over, the one named last changes fastest.
Arguments:
- grads: bfloat16 [2, 16, 128, 6144], P('expert', 'dp'), may hold values from -16 to 16
- master: float32 [2, 128, 6144], P('expert', 'dp'), may hold values from -0.0625 to 0.0625
- first_moment: float32 [2, 128, 6144], P('expert', 'dp'), may hold values from -0.0029296875 to 0.0029296875
- second_moment: float32 [2, 128, 6144], P('expert', 'dp'), may hold values from 1e-08 to 1e-07
Outputs:
- new_master: float32 [2, 128, 6144], P('expert', 'dp')
- new_first: float32 [2, 128, 6144], P('expert', 'dp')
- new_second: float32 [2, 128, 6144], P('expert', 'dp')
- direction: float32 [2, 128, 6144], P('expert', 'dp')
- new_weights: bfloat16 [2, 128, 6144], P('expert')
The draws below stay inside these ranges and needn't reach their ends.
All inputs are finite; a program needn't handle non-finite values.
Results may differ from the reference program's by a relative error of at most 0.0004.
Values may be sent and summed in bfloat16 or wider, within the bound.
No kernel may reach another device: no remote copies, remote signals or barrier semaphores. Data moves between devices by JAX's collectives and lax.ppermute only.
A program may use at most 64 MiB of HBM per device.

```python
import math
import jax
import jax.numpy as jnp
from jax import lax

D = 6144
ROWS = 128
STEP = 10
EXPERTS = 2
N_DP = 16


def draw_grads(key, part):
    key_common = jax.random.fold_in(key, 11)
    key_scale = jax.random.fold_in(key, 12)
    key_noise = jax.random.fold_in(key, 13)
    key_pairs = jax.random.fold_in(key, 14)
    rows_per = ROWS // N_DP
    row_scale = jnp.exp(jax.random.uniform(key_scale, (EXPERTS, 1, ROWS, 1), jnp.float32, math.log(0.5), math.log(2.0)))
    pairing = jax.random.permutation(key_pairs, N_DP)
    owner = jnp.arange(ROWS, dtype=jnp.int32) // rows_per
    spike = jnp.where(owner[None, :] == pairing[:, None], 4.0, 1.0).astype(jnp.float32)
    spike = spike.reshape(1, N_DP, ROWS, 1)
    common = 0.25 * row_scale * jax.random.truncated_normal(key_common, -4.0, 4.0, (EXPERTS, 1, ROWS, D), jnp.float32)
    noise = jax.random.truncated_normal(key_noise, -3.0, 3.0, (EXPERTS, N_DP, ROWS, D), jnp.float32)
    return (common + spike * noise).astype(jnp.bfloat16)


def block_levels(key, extent, cuts, least, largest):
    gain = 1.0
    for axis_at, parts in cuts:
        steps = jax.random.uniform(jax.random.fold_in(jax.random.fold_in(key, 6), axis_at), (parts,), jnp.float32, least / len(cuts), largest / len(cuts))
        gain = gain * jnp.repeat(jnp.exp(steps), extent[axis_at] // parts).reshape((-1,) + (1,) * (len(extent) - 1 - axis_at))
    return gain


def normal_values(stream_key, extent, deviation, most, shards=(), held_as=jnp.bfloat16):
    result = deviation * jax.random.normal(stream_key, extent, jnp.float32)
    if shards:
        result = result * block_levels(stream_key, extent, shards, -0.22, 0.18)
    return jnp.clip(result, -most, most).astype(held_as)


def setup_inputs(seed: int = 0) -> dict:
    seeds = jax.random.split(jax.random.key(seed), 5)
    return {
        "grads": draw_grads(jax.random.fold_in(seeds[4], 71), 0),
        "master": normal_values(seeds[1], (EXPERTS, ROWS, D), 0.004, 0.0625, ((0, 2), (1, 16)), jnp.float32),
        "first_moment": normal_values(seeds[2], (EXPERTS, ROWS, D), 0.0002, 0.0029296875, ((0, 2), (1, 16)), jnp.float32),
        "second_moment": jnp.clip(jnp.exp(math.log(1.0000000116860974e-07) - 2.3025851 * jax.random.uniform(seeds[3], (EXPERTS, ROWS, D), jnp.float32) ** block_levels(seeds[3], (EXPERTS, ROWS, D), ((0, 2), (1, 16)), -0.2, 0.2)), 9.99999993922529e-09, 1.0000000116860974e-07),
    }


def reference(grads, master, first_moment, second_moment):

    def add_one(index, total):
        piece = lax.dynamic_index_in_dim(grads, index, 1, keepdims=False)
        return total + piece.astype(jnp.float32)
    summed = lax.fori_loop(0, grads.shape[1], add_one, jnp.zeros(master.shape, jnp.float32))
    norm = jnp.sqrt(jnp.sum(summed * summed))
    clip = 1.0 / jnp.maximum(norm, 1.0)
    clipped = clip * summed
    new_first = 0.9 * first_moment + 0.1 * clipped
    new_second = 0.95 * second_moment + 0.05 * (clipped * clipped)
    first_fix = 1.0 - 0.9 ** STEP
    second_fix = 1.0 - 0.95 ** STEP
    direction = new_first / first_fix / (jnp.sqrt(new_second / second_fix) + 1e-08)
    new_master = master - 0.001 * (direction + 0.1 * master)
    new_weights = new_master.astype(jnp.bfloat16)
    return (new_master, new_first, new_second, direction, new_weights)
```

```python
import jax
import jax.numpy as jnp
from jax import lax
from jax.sharding import PartitionSpec as P

STEP = 10


def _swap(size, offset):
    return [(i, i ^ offset) for i in range(size)]


def _pick(array, index):
    return lax.dynamic_index_in_dim(array, index, 0, keepdims=False)


def shards(size, grads, master, first_moment, second_moment):
    rows, width = master.shape[1:]
    near = 4 if size % 4 == 0 else 1
    far = size // near
    me = lax.axis_index("dp")
    far_at, near_at = me // near, me % near

    blocks = grads[0, 0].reshape(far, near, rows, width)
    sums = []
    for k in reversed(range(far)):
        group = _pick(blocks, far_at ^ k)
        total = _pick(group, near_at).astype(jnp.float32)
        for j in reversed(range(1, near)):
            moved = lax.ppermute(_pick(group, near_at ^ j), "dp", _swap(size, j))
            total = total + moved.astype(jnp.float32)
        sums.append(total)
    summed = sums[-1]
    for k, total in zip(reversed(range(1, far)), sums):
        summed = summed + lax.ppermute(total, "dp", _swap(size, k * near))

    devices = size * lax.axis_size("expert")
    square = jnp.broadcast_to(jnp.sum(summed * summed), (devices, 8, 128))
    squares = lax.all_to_all(square, ("expert", "dp"), 0, 0)
    norm = jnp.sqrt(jnp.sum(squares[:, 0, 0]))
    clip = 1.0 / jnp.maximum(norm, 1.0)
    clipped = clip * summed
    new_first = 0.9 * first_moment[0] + 0.1 * clipped
    new_second = 0.95 * second_moment[0] + 0.05 * (clipped * clipped)
    first_fix = 1.0 - 0.9**STEP
    second_fix = 1.0 - 0.95**STEP
    direction = new_first / first_fix / (jnp.sqrt(new_second / second_fix) + 1e-08)
    new_master = master[0] - 0.001 * (direction + 0.1 * master[0])

    own = new_master.astype(jnp.bfloat16)
    held = [own]
    for k in range(2, size, 2):
        held.append(lax.ppermute(own, "dp", _swap(size, k)))
    held = jnp.stack(held)
    other = lax.ppermute(held, "dp", _swap(size, 1))
    full = jnp.stack([held, other], 1).reshape(size, rows, width)
    full = jnp.take(full, jnp.arange(size) ^ me, axis=0)
    new_weights = full.reshape(1, size * rows, width)
    return (new_master[None], new_first[None], new_second[None], direction[None], new_weights)


def solution(mesh):
    state = P("expert", "dp", None)
    return jax.shard_map(
        lambda *args: shards(mesh.shape["dp"], *args),
        mesh=mesh,
        in_specs=(P("expert", "dp", None, None), state, state, state),
        out_specs=(state, state, state, state, P("expert", None, None)),
        check_vma=False,
    )
```

```python
import jax
import jax.numpy as jnp
from jax import lax
from jax.sharding import PartitionSpec as P

STEP = 10
NEAR = 4


def _swap(array, size, offset):
    return lax.ppermute(array, "dp", [(i, i ^ offset) for i in range(size)])


def _pick(array, index):
    return lax.dynamic_index_in_dim(array, index, 0, keepdims=False)


def _sum_rows(grads, rows, width, size):
    far = size // NEAR
    me = lax.axis_index("dp")
    far_at, near_at = me // NEAR, me % NEAR
    blocks = grads.reshape(far, NEAR, rows, width)
    order = list(reversed(range(far)))
    pieces = []
    for k in order:
        group = _pick(blocks, far_at ^ k)
        pieces.append([_pick(group, near_at ^ j) for j in range(NEAR)])
    pieces = lax.optimization_barrier(pieces)
    moved = []
    for k, piece in zip(order, pieces):
        moved.append([_swap(piece[j], size, j) for j in (2, 3, 1)])
    sums = []
    for k, piece, others in zip(order, pieces, moved):
        total = piece[0].astype(jnp.float32)
        for other in others:
            total = total + other.astype(jnp.float32)
        sums.append(total)
    summed = sums[-1]
    for k, total in zip(order[:-1], sums):
        other = _swap(total, size, k * NEAR)
        summed = summed + other
    return summed


def shards(size, grads, master, first_moment, second_moment):
    rows, width = master.shape[1:]
    me = lax.axis_index("dp")
    summed = _sum_rows(grads[0, 0], rows, width, size)

    devices = size * lax.axis_size("expert")
    square = jnp.broadcast_to(jnp.sum(summed * summed), (devices, 1, 128))
    squares = lax.all_to_all(square, ("expert", "dp"), 0, 0)
    norm = jnp.sqrt(jnp.sum(squares[:, 0, 0]))
    clip = 1.0 / jnp.maximum(norm, 1.0)
    clipped = clip * summed
    new_first = 0.9 * first_moment[0] + 0.1 * clipped
    new_second = 0.95 * second_moment[0] + 0.05 * (clipped * clipped)
    first_fix = 1.0 - 0.9**STEP
    second_fix = 1.0 - 0.95**STEP
    direction = new_first / first_fix / (jnp.sqrt(new_second / second_fix) + 1e-08)
    new_master = master[0] - 0.001 * (direction + 0.1 * master[0])

    own = new_master.astype(jnp.bfloat16)
    held = [own]
    for k in range(2, size, 2):
        held.append(_swap(own, size, k))
    held = jnp.stack(held)
    other = _swap(held, size, 1)
    full = jnp.stack([held, other], 1).reshape(size, rows, width)
    full = jnp.take(full, jnp.arange(size) ^ me, axis=0)
    new_weights = full.reshape(1, size * rows, width)
    return (new_master[None], new_first[None], new_second[None], direction[None], new_weights)


def solution(mesh):
    state = P("expert", "dp", None)
    size = mesh.shape["dp"]
    return jax.shard_map(
        lambda *args: shards(size, *args),
        mesh=mesh,
        in_specs=(P("expert", "dp", None, None), state, state, state),
        out_specs=(state, state, state, state, P("expert", None, None)),
        check_vma=False,
    )
```

```python
import functools

import jax
import jax.numpy as jnp
from jax import lax
from jax.experimental import pallas as pl
from jax.experimental.pallas import tpu as pltpu
from jax.sharding import PartitionSpec as P

STEP = 10
NEAR = 4
VMEM = pl.BlockSpec(memory_space=pltpu.VMEM)


def _swap(array, size, offset):
    return lax.ppermute(array, "dp", [(i, i ^ offset) for i in range(size)])


def _pick(array, index):
    return lax.dynamic_index_in_dim(array, index, 0, keepdims=False)


def _call(body, outs, *args):
    return pl.pallas_call(
        body,
        out_shape=outs,
        in_specs=[VMEM] * len(args),
        out_specs=[VMEM] * len(outs),
        cost_estimate=pl.CostEstimate(flops=1000000, bytes_accessed=1000000, transcendentals=0),
    )(*(pltpu.with_memory_space_constraint(arg, pltpu.VMEM) for arg in args))


def _far_order(size):
    far = size // NEAR
    return [far - 2, far - 1, *reversed(range(far - 2))]


def _near_sums(grads, rows, width, size):
    far = size // NEAR
    me = lax.axis_index("dp")
    far_at, near_at = me // NEAR, me % NEAR
    blocks = grads.reshape(far, NEAR, rows, width)
    order = _far_order(size)
    pieces = []
    for k in order:
        group = _pick(blocks, far_at ^ k)
        pieces.append([_pick(group, near_at ^ j) for j in range(NEAR)])
    pieces = lax.optimization_barrier(pieces)
    moved = []
    for k, piece in zip(order, pieces):
        moved.append([_swap(piece[j], size, j) for j in (2, 3, 1)])
    sums = {}
    for k, piece, others in zip(order, pieces, moved):
        total = piece[0].astype(jnp.float32)
        for other in others:
            total = total + other.astype(jnp.float32)
        sums[k] = total
    return sums


def _finish_sum(*refs):
    *parts, summed, square = refs
    total = parts[0][...]
    for part in parts[1:]:
        total = total + part[...]
    summed[...] = total
    own = jnp.sum(jnp.sum(total * total, axis=1, keepdims=True), axis=0, keepdims=True)
    square[...] = jnp.broadcast_to(own[None], square.shape)


def _update(squares, summed, master, first, second):
    norm = jnp.sqrt(jnp.sum(squares[...], axis=0))[:, :1]
    clip = 1.0 / jnp.maximum(norm, 1.0)
    clipped = clip * summed[...]
    new_first = 0.9 * first[...] + 0.1 * clipped
    new_second = 0.95 * second[...] + 0.05 * (clipped * clipped)
    first_fix = 1.0 - 0.9**STEP
    second_fix = 1.0 - 0.95**STEP
    direction = new_first / first_fix / (jnp.sqrt(new_second / second_fix) + 1e-08)
    new_master = master[...] - 0.001 * (direction + 0.1 * master[...])
    return new_master, new_first, new_second, direction


def _weights(squares, summed, master, first, second, own):
    own[...] = _update(squares, summed, master, first, second)[0].astype(jnp.bfloat16)


def _states(squares, summed, master, first, second, *outs):
    for out, value in zip(outs, _update(squares, summed, master, first, second)):
        out[...] = value


def _place(size, *refs):
    *groups, out, done = refs
    me = lax.axis_index("dp")
    far = size // NEAR
    copies = []
    for g, group in enumerate(groups):
        for k in range(far):
            offset = k * NEAR + g
            copies.append(pltpu.make_async_copy(group.at[k], out.at[me ^ offset], done.at[offset]))
    for copy in copies:
        copy.start()
    for copy in copies:
        copy.wait()


def _step(size, grads, master, first, second):
    rows, width = master.shape
    f32 = jax.ShapeDtypeStruct((rows, width), jnp.float32)
    order = _far_order(size)
    sums = _near_sums(grads, rows, width, size)
    parts = [sums[0]]
    for k in order[:-1]:
        parts.append(_swap(sums[k], size, k * NEAR))

    devices = size * lax.axis_size("expert")
    kept = pltpu.VMEM((rows, width), jnp.float32)
    square = pltpu.VMEM((devices, 1, 128), jnp.float32)
    summed, square = _call(_finish_sum, (kept, square), *parts)
    squares = lax.all_to_all(square, ("expert", "dp"), 0, 0)
    state = (squares, summed, master, first, second)
    (own,) = _call(_weights, (pltpu.VMEM((rows, width), jnp.bfloat16),), *state)
    results = _call(_states, (f32,) * 4, *state)

    here, there = {0: own}, {}
    for k in order[:-1]:
        here[k] = _swap(own, size, k * NEAR)
    for k in (0, *order[:-1]):
        there[k] = _swap(here[k], size, 2)
    here = jnp.stack([here[k] for k in range(size // NEAR)])
    there = jnp.stack([there[k] for k in range(size // NEAR)])
    here_pair = _swap(here, size, 1)
    there_pair = _swap(there, size, 1)
    new_weights = pl.pallas_call(
        functools.partial(_place, size),
        out_shape=jax.ShapeDtypeStruct((size, rows, width), jnp.bfloat16),
        in_specs=[VMEM] * 4,
        out_specs=pl.BlockSpec(memory_space=pl.ANY),
        scratch_shapes=[pltpu.SemaphoreType.DMA((size,))],
    )(*(pltpu.with_memory_space_constraint(x, pltpu.VMEM) for x in (here, here_pair, there, there_pair)))
    return results, new_weights


def shards(size, grads, master, first_moment, second_moment):
    results, new_weights = _step(size, grads[0, 0], master[0], first_moment[0], second_moment[0])
    new_weights = new_weights.reshape(1, -1, master.shape[2])
    return (*(result[None] for result in results), new_weights)


def solution(mesh):
    state = P("expert", "dp", None)
    size = mesh.shape["dp"]
    return jax.shard_map(
        functools.partial(shards, size),
        mesh=mesh,
        in_specs=(P("expert", "dp", None, None), state, state, state),
        out_specs=(state, state, state, state, P("expert", None, None)),
        check_vma=False,
    )
```

```python
import functools

import jax
import jax.numpy as jnp
from jax import lax
from jax.experimental import pallas as pl
from jax.experimental.pallas import tpu as pltpu
from jax.sharding import PartitionSpec as P

STEP = 10
NEAR = 4
VMEM = pl.BlockSpec(memory_space=pltpu.VMEM)


def _swap(array, size, offset):
    return lax.ppermute(array, "dp", [(i, i ^ offset) for i in range(size)])


def _pick(array, index):
    return lax.dynamic_index_in_dim(array, index, 0, keepdims=False)


def _call(body, outs, *args):
    return pl.pallas_call(
        body,
        out_shape=outs,
        in_specs=[VMEM] * len(args),
        out_specs=[VMEM] * len(outs),
        cost_estimate=pl.CostEstimate(flops=1000000, bytes_accessed=1000000, transcendentals=0),
    )(*(pltpu.with_memory_space_constraint(arg, pltpu.VMEM) for arg in args))


def _groups(size):
    far = size // NEAR
    return [[far - 2], list(reversed(range(1, far - 2))), [far - 1], [0]]


def _far_order(size):
    return [k for group in _groups(size) for k in group]


def _outward(size):
    far = size // NEAR
    return [far // 2, *(k for k in range(1, far) if k != far // 2)]


def _near_sums(grads, rows, width, size):
    far = size // NEAR
    me = lax.axis_index("dp")
    far_at, near_at = me // NEAR, me % NEAR

    def piece(grads, offsets, j):
        blocks = grads.reshape(far, NEAR, rows, width)
        return jnp.stack([_pick(_pick(blocks, far_at ^ k), near_at ^ j) for k in offsets])

    groups = _groups(size)
    order = _far_order(size)
    first = lax.optimization_barrier([piece(grads, groups[0], j) for j in (2, 3)])
    grads, _ = lax.optimization_barrier((grads, first))
    own, pair = piece(grads, order, 0), piece(grads, order, 1)
    rest = [[piece(grads, group, j) for j in (2, 3)] for group in groups[1:]]
    own, pair, rest = lax.optimization_barrier((own, pair, rest))
    moved = []
    for pieces in [first, *rest]:
        moved.append([_swap(pieces[0], size, 2), _swap(pieces[1], size, 3)])
    pair = _swap(pair, size, 1)
    sums = {}
    block = pltpu.VMEM((rows, width), jnp.float32)
    for g, group in enumerate(groups):
        at = [order.index(k) for k in group]
        totals = _call(functools.partial(_add_near, at), (block,) * len(at), own, pair, *moved[g])
        sums.update(zip(group, totals))
    return sums


def _add_near(at, own, pair, left, right, *totals):
    for i, (k, total) in enumerate(zip(at, totals)):
        here = own[k].astype(jnp.float32) + pair[k].astype(jnp.float32)
        total[...] = here + left[i].astype(jnp.float32) + right[i].astype(jnp.float32)


def _finish_sum(*refs):
    *parts, summed, square = refs
    total = parts[0][...]
    for part in parts[1:]:
        total = total + part[...]
    summed[...] = total
    own = jnp.sum(jnp.sum(total * total, axis=1, keepdims=True), axis=0, keepdims=True)
    square[...] = jnp.broadcast_to(own[None], square.shape)


def _update(squares, summed, master, first, second):
    norm = jnp.sqrt(jnp.sum(squares[...], axis=0))[:, :1]
    clip = 1.0 / jnp.maximum(norm, 1.0)
    clipped = clip * summed[...]
    new_first = 0.9 * first[...] + 0.1 * clipped
    new_second = 0.95 * second[...] + 0.05 * (clipped * clipped)
    first_fix = 1.0 - 0.9**STEP
    second_fix = 1.0 - 0.95**STEP
    direction = new_first / first_fix / (jnp.sqrt(new_second / second_fix) + 1e-08)
    new_master = master[...] - 0.001 * (direction + 0.1 * master[...])
    return new_master, new_first, new_second, direction


def _weights(squares, summed, master, first, second, own):
    own[...] = _update(squares, summed, master, first, second)[0].astype(jnp.bfloat16)


def _states(squares, summed, master, first, second, *outs):
    for out, value in zip(outs, _update(squares, summed, master, first, second)):
        out[...] = value


def _place(offsets, blocks, *refs):
    *_, out, done = refs
    me = lax.axis_index("dp")
    copies = [
        pltpu.make_async_copy(block, out.at[me ^ offset], done.at[i])
        for i, (offset, block) in enumerate(zip(offsets, blocks))
    ]
    for copy in copies:
        copy.start()
    for copy in copies:
        copy.wait()


def _placed(size, blocks, *rows):
    offsets = list(blocks)
    height, width = blocks[offsets[0]].shape

    def body(*refs):
        _place(offsets, refs[: len(offsets)], *refs[len(offsets) :])

    return pl.pallas_call(
        body,
        out_shape=jax.ShapeDtypeStruct((size, height, width), jnp.bfloat16),
        in_specs=[VMEM] * len(offsets) + [pl.BlockSpec(memory_space=pl.ANY)] * len(rows),
        out_specs=pl.BlockSpec(memory_space=pl.ANY),
        scratch_shapes=[pltpu.SemaphoreType.DMA((len(offsets),))],
        input_output_aliases={len(offsets): 0} if rows else {},
        cost_estimate=pl.CostEstimate(flops=1000000, bytes_accessed=1000000, transcendentals=0),
    )(*(pltpu.with_memory_space_constraint(block, pltpu.VMEM) for block in blocks.values()), *rows)


def _step(size, grads, master, first, second):
    rows, width = master.shape
    f32 = jax.ShapeDtypeStruct((rows, width), jnp.float32)
    order = _far_order(size)
    sums = _near_sums(grads, rows, width, size)
    parts = [sums[0]]
    for k in order[:-1]:
        parts.append(_swap(sums[k], size, k * NEAR))

    devices = size * lax.axis_size("expert")
    kept = pltpu.VMEM((rows, width), jnp.float32)
    square = pltpu.VMEM((devices, 1, 128), jnp.float32)
    summed, square = _call(_finish_sum, (kept, square), *parts)
    squares = lax.all_to_all(square, ("expert", "dp"), 0, 0)
    state = (squares, summed, master, first, second)
    (own,) = _call(_weights, (pltpu.VMEM((rows, width), jnp.bfloat16),), *state)
    results = _call(_states, (f32,) * 4, *state)

    blocks = {0: own}
    for k in _outward(size):
        blocks[k * NEAR] = _swap(own, size, k * NEAR)
    for k in (0, *_outward(size)):
        blocks[k * NEAR + 2] = _swap(blocks[k * NEAR], size, 2)
    for offset in list(blocks):
        blocks[offset + 1] = _swap(blocks[offset], size, 1)
    last = size - 1
    early = {k: block for k, block in blocks.items() if not k & 2}
    late = {k: block for k, block in blocks.items() if k & 2 and k != last}
    placed = _placed(size, early)
    placed = _placed(size, late, placed)
    new_weights = _placed(size, {last: blocks[last]}, placed)
    return results, new_weights


def shards(size, grads, master, first_moment, second_moment):
    results, new_weights = _step(size, grads[0, 0], master[0], first_moment[0], second_moment[0])
    new_weights = new_weights.reshape(1, -1, master.shape[2])
    return (*(result[None] for result in results), new_weights)


def solution(mesh):
    state = P("expert", "dp", None)
    size = mesh.shape["dp"]
    return jax.shard_map(
        functools.partial(shards, size),
        mesh=mesh,
        in_specs=(P("expert", "dp", None, None), state, state, state),
        out_specs=(state, state, state, state, P("expert", None, None)),
        check_vma=False,
    )
```

```python
import functools

import jax
import jax.numpy as jnp
from jax import lax
from jax.experimental import pallas as pl
from jax.experimental.pallas import tpu as pltpu
from jax.sharding import PartitionSpec as P

STEP = 10
NEAR = 4
VMEM = pl.BlockSpec(memory_space=pltpu.VMEM)


def _swap(array, size, offset):
    return lax.ppermute(array, "dp", [(i, i ^ offset) for i in range(size)])


def _hop(array, moves):
    near = range(NEAR)
    return lax.ppermute(array, "dp", [(a * NEAR + j, b * NEAR + j) for a, b in moves.items() for j in near])


def _pick(array, index):
    return lax.dynamic_index_in_dim(array, index, 0, keepdims=False)


def _call(body, outs, *args):
    return pl.pallas_call(
        body,
        out_shape=outs,
        in_specs=[VMEM] * len(args),
        out_specs=[VMEM] * len(outs),
        cost_estimate=pl.CostEstimate(flops=1000000, bytes_accessed=1000000, transcendentals=0),
    )(*(pltpu.with_memory_space_constraint(arg, pltpu.VMEM) for arg in args))


def _groups(size):
    far = size // NEAR
    return [[far - 1], [far - 2], list(reversed(range(1, far - 2))), [0]]


def _far_order(size):
    return [k for group in _groups(size) for k in group]


def _outward(size):
    far = size // NEAR
    return [3, 1, 2] if far == 4 else list(range(1, far))


def _near_sums(grads, rows, width, size):
    far = size // NEAR
    me = lax.axis_index("dp")
    far_at, near_at = me // NEAR, me % NEAR

    def piece(grads, offsets, j):
        blocks = grads.reshape(far, NEAR, rows, width)
        return jnp.stack([_pick(_pick(blocks, far_at ^ k), near_at ^ j) for k in offsets])

    groups = _groups(size)
    order = _far_order(size)
    first = lax.optimization_barrier([piece(grads, groups[0], j) for j in (2, 3)])
    grads, _ = lax.optimization_barrier((grads, first))
    own, pair = piece(grads, order, 0), piece(grads, order, 1)
    rest = [[piece(grads, group, j) for j in (2, 3)] for group in groups[1:]]
    own, pair, rest = lax.optimization_barrier((own, pair, rest))
    moved = []
    for pieces in [first, *rest]:
        moved.append([_swap(pieces[0], size, 2), _swap(pieces[1], size, 3)])
    pair = _swap(pair, size, 1)
    sums = {}
    block = pltpu.VMEM((rows, width), jnp.float32)
    for g, group in enumerate(groups):
        at = [order.index(k) for k in group]
        totals = _call(functools.partial(_add_near, at), (block,) * len(at), own, pair, *moved[g])
        sums.update(zip(group, totals))
    return sums


def _add_near(at, own, pair, left, right, *totals):
    for i, (k, total) in enumerate(zip(at, totals)):
        here = own[k].astype(jnp.float32) + pair[k].astype(jnp.float32)
        total[...] = here + left[i].astype(jnp.float32) + right[i].astype(jnp.float32)


def _far_sums(sums, size):
    far = size // NEAR
    parts = []
    order = _far_order(size)[:-1]
    if far == 4:
        relayed = _hop(sums[3], {3: 2, 0: 1})
        parts.append(_hop(sums[3], {2: 1, 1: 2}))
        (joined,) = _call(_add, (pltpu.VMEM(sums[2].shape, jnp.float32),), sums[2], relayed)
        sums = {**sums, 2: joined}
        order = order[1:]
    for k in order:
        parts.append(_swap(sums[k], size, k * NEAR))
    return parts


def _add(left, right, total):
    total[...] = left[...] + right[...]


def _finish_sum(*refs):
    *parts, summed, square = refs
    total = parts[0][...]
    for part in parts[1:]:
        total = total + part[...]
    summed[...] = total
    own = jnp.sum(jnp.sum(total * total, axis=1, keepdims=True), axis=0, keepdims=True)
    square[...] = jnp.broadcast_to(own[None], square.shape)


def _update(squares, summed, master, first, second):
    norm = jnp.sqrt(jnp.sum(squares[...], axis=0))[:, :1]
    clip = 1.0 / jnp.maximum(norm, 1.0)
    clipped = clip * summed[...]
    new_first = 0.9 * first[...] + 0.1 * clipped
    new_second = 0.95 * second[...] + 0.05 * (clipped * clipped)
    first_fix = 1.0 - 0.9**STEP
    second_fix = 1.0 - 0.95**STEP
    direction = new_first / first_fix / (jnp.sqrt(new_second / second_fix) + 1e-08)
    new_master = master[...] - 0.001 * (direction + 0.1 * master[...])
    return new_master, new_first, new_second, direction


def _weights(squares, summed, master, first, second, own):
    own[...] = _update(squares, summed, master, first, second)[0].astype(jnp.bfloat16)


def _states(squares, summed, master, first, second, *outs):
    for out, value in zip(outs, _update(squares, summed, master, first, second)):
        out[...] = value


def _place(offsets, blocks, *refs):
    *_, out, done = refs
    me = lax.axis_index("dp")
    copies = [
        pltpu.make_async_copy(block, out.at[me ^ offset], done.at[i])
        for i, (offset, block) in enumerate(zip(offsets, blocks))
    ]
    for copy in copies:
        copy.start()
    for copy in copies:
        copy.wait()


def _placed(size, blocks, *rows):
    offsets = list(blocks)
    height, width = blocks[offsets[0]].shape

    def body(*refs):
        _place(offsets, refs[: len(offsets)], *refs[len(offsets) :])

    return pl.pallas_call(
        body,
        out_shape=jax.ShapeDtypeStruct((size, height, width), jnp.bfloat16),
        in_specs=[VMEM] * len(offsets) + [pl.BlockSpec(memory_space=pl.ANY)] * len(rows),
        out_specs=pl.BlockSpec(memory_space=pl.ANY),
        scratch_shapes=[pltpu.SemaphoreType.DMA((len(offsets),))],
        input_output_aliases={len(offsets): 0} if rows else {},
        cost_estimate=pl.CostEstimate(flops=1000000, bytes_accessed=1000000, transcendentals=0),
    )(*(pltpu.with_memory_space_constraint(block, pltpu.VMEM) for block in blocks.values()), *rows)


def _step(size, grads, master, first, second):
    rows, width = master.shape
    f32 = jax.ShapeDtypeStruct((rows, width), jnp.float32)
    sums = _near_sums(grads, rows, width, size)
    parts = [sums[0], *_far_sums(sums, size)]

    devices = size * lax.axis_size("expert")
    kept = pltpu.VMEM((rows, width), jnp.float32)
    square = pltpu.VMEM((devices, 1, 128), jnp.float32)
    summed, square = _call(_finish_sum, (kept, square), *parts)
    squares = lax.all_to_all(square, ("expert", "dp"), 0, 0)
    state = (squares, summed, master, first, second)
    (own,) = _call(_weights, (pltpu.VMEM((rows, width), jnp.bfloat16),), *state)
    results = _call(_states, (f32,) * 4, *state)

    blocks = {0: own}
    for k in _outward(size):
        blocks[k * NEAR] = _swap(own, size, k * NEAR)
    for k in (0, *_outward(size)):
        blocks[k * NEAR + 2] = _swap(blocks[k * NEAR], size, 2)
    for offset in list(blocks):
        blocks[offset + 1] = _swap(blocks[offset], size, 1)
    placed = _placed(size, {k: block for k, block in blocks.items() if not k & 2})
    placed = _placed(size, {k: block for k, block in blocks.items() if k & 3 == 2}, placed)
    new_weights = _placed(size, {k: block for k, block in blocks.items() if k & 3 == 3}, placed)
    return results, new_weights


def shards(size, grads, master, first_moment, second_moment):
    results, new_weights = _step(size, grads[0, 0], master[0], first_moment[0], second_moment[0])
    new_weights = new_weights.reshape(1, -1, master.shape[2])
    return (*(result[None] for result in results), new_weights)


def solution(mesh):
    state = P("expert", "dp", None)
    size = mesh.shape["dp"]
    return jax.shard_map(
        functools.partial(shards, size),
        mesh=mesh,
        in_specs=(P("expert", "dp", None, None), state, state, state),
        out_specs=(state, state, state, state, P("expert", None, None)),
        check_vma=False,
    )
```

```python
import functools

import jax
import jax.numpy as jnp
from jax import lax
from jax.experimental import pallas as pl
from jax.experimental.pallas import tpu as pltpu
from jax.sharding import PartitionSpec as P

STEP = 10
NEAR = 4
VMEM = pl.BlockSpec(memory_space=pltpu.VMEM)


def _swap(array, size, offset):
    return lax.ppermute(array, "dp", [(i, i ^ offset) for i in range(size)])


def _hop(array, moves):
    near = range(NEAR)
    return lax.ppermute(array, "dp", [(a * NEAR + j, b * NEAR + j) for a, b in moves.items() for j in near])


def _call(body, outs, *args):
    return pl.pallas_call(
        body,
        out_shape=outs,
        in_specs=[VMEM] * len(args),
        out_specs=[VMEM] * len(outs),
        cost_estimate=pl.CostEstimate(flops=1000000, bytes_accessed=1000000, transcendentals=0),
    )(*(pltpu.with_memory_space_constraint(arg, pltpu.VMEM) for arg in args))


def _groups(size):
    far = size // NEAR
    return [[far - 1], [far - 2], list(reversed(range(1, far - 2))), [0]]


def _far_order(size):
    return [k for group in _groups(size) for k in group]


def _outward(size):
    far = size // NEAR
    return [3, 1, 2] if far == 4 else list(range(1, far))


def _copy_rows(wanted, blocks, *refs):
    *outs, done = refs
    me = lax.axis_index("dp")
    copies = []
    for offsets, out in zip(wanted, outs):
        for i, offset in enumerate(offsets):
            copies.append(pltpu.make_async_copy(blocks.at[me ^ offset], out.at[i], done.at[len(copies)]))
    for copy in copies:
        copy.start()
    for copy in copies:
        copy.wait()


def _cut(blocks, wanted):
    _, rows, width = blocks.shape
    return pl.pallas_call(
        functools.partial(_copy_rows, wanted),
        out_shape=[pltpu.VMEM((len(offsets), rows, width), blocks.dtype) for offsets in wanted],
        in_specs=[pl.BlockSpec(memory_space=pl.ANY)],
        out_specs=[VMEM] * len(wanted),
        scratch_shapes=[pltpu.SemaphoreType.DMA((sum(map(len, wanted)),))],
        cost_estimate=pl.CostEstimate(flops=1000000, bytes_accessed=1000000, transcendentals=0),
    )(pltpu.with_memory_space_constraint(blocks, pltpu.HBM))


def _near_sums(grads, rows, width, size):
    blocks = grads.reshape(size, rows, width)
    groups = _groups(size)
    order = _far_order(size)
    first = _cut(blocks, [[k * NEAR + j for k in groups[0]] for j in (2, 3)])
    wanted = [[k * NEAR + j for k in group] for group in groups[1:] for j in (2, 3)]
    rest = _cut(blocks, [[k * NEAR + j for k in order] for j in (0, 1)] + wanted)
    own, pair, *rest = rest
    rest = list(zip(rest[::2], rest[1::2]))
    moved = []
    for pieces in [first, *rest]:
        moved.append([_swap(pieces[0], size, 2), _swap(pieces[1], size, 3)])
    pair = _swap(pair, size, 1)
    sums = {}
    block = pltpu.VMEM((rows, width), jnp.float32)
    for g, group in enumerate(groups):
        at = [order.index(k) for k in group]
        totals = _call(functools.partial(_add_near, at), (block,) * len(at), own, pair, *moved[g])
        sums.update(zip(group, totals))
    return sums


def _add_near(at, own, pair, left, right, *totals):
    for i, (k, total) in enumerate(zip(at, totals)):
        here = own[k].astype(jnp.float32) + pair[k].astype(jnp.float32)
        total[...] = here + left[i].astype(jnp.float32) + right[i].astype(jnp.float32)


def _far_sums(sums, size):
    far = size // NEAR
    parts = []
    order = _far_order(size)[:-1]
    if far == 4:
        relayed = _hop(sums[3], {3: 2, 0: 1})
        parts.append(_hop(sums[3], {2: 1, 1: 2}))
        (joined,) = _call(_add, (pltpu.VMEM(sums[2].shape, jnp.float32),), sums[2], relayed)
        sums = {**sums, 2: joined}
        order = order[1:]
    for k in order:
        parts.append(_swap(sums[k], size, k * NEAR))
    return parts


def _add(left, right, total):
    total[...] = left[...] + right[...]


def _finish_sum(*refs):
    *parts, summed, square = refs
    total = parts[0][...]
    for part in parts[1:]:
        total = total + part[...]
    summed[...] = total
    own = jnp.sum(jnp.sum(total * total, axis=1, keepdims=True), axis=0, keepdims=True)
    square[...] = jnp.broadcast_to(own[None], square.shape)


def _update(squares, summed, master, first, second):
    norm = jnp.sqrt(jnp.sum(squares[...], axis=0))[:, :1]
    clip = 1.0 / jnp.maximum(norm, 1.0)
    clipped = clip * summed[...]
    new_first = 0.9 * first[...] + 0.1 * clipped
    new_second = 0.95 * second[...] + 0.05 * (clipped * clipped)
    first_fix = 1.0 - 0.9**STEP
    second_fix = 1.0 - 0.95**STEP
    direction = new_first / first_fix / (jnp.sqrt(new_second / second_fix) + 1e-08)
    new_master = master[...] - 0.001 * (direction + 0.1 * master[...])
    return new_master, new_first, new_second, direction


def _weights(squares, summed, master, first, second, own):
    own[...] = _update(squares, summed, master, first, second)[0].astype(jnp.bfloat16)


def _states(squares, summed, master, first, second, *outs):
    for out, value in zip(outs, _update(squares, summed, master, first, second)):
        out[...] = value


def _place(offsets, blocks, *refs):
    *_, out, done = refs
    me = lax.axis_index("dp")
    copies = [
        pltpu.make_async_copy(block, out.at[me ^ offset], done.at[i])
        for i, (offset, block) in enumerate(zip(offsets, blocks))
    ]
    for copy in copies:
        copy.start()
    for copy in copies:
        copy.wait()


def _placed(size, blocks, *rows):
    offsets = list(blocks)
    height, width = blocks[offsets[0]].shape

    def body(*refs):
        _place(offsets, refs[: len(offsets)], *refs[len(offsets) :])

    return pl.pallas_call(
        body,
        out_shape=jax.ShapeDtypeStruct((size, height, width), jnp.bfloat16),
        in_specs=[VMEM] * len(offsets) + [pl.BlockSpec(memory_space=pl.ANY)] * len(rows),
        out_specs=pl.BlockSpec(memory_space=pl.ANY),
        scratch_shapes=[pltpu.SemaphoreType.DMA((len(offsets),))],
        input_output_aliases={len(offsets): 0} if rows else {},
        cost_estimate=pl.CostEstimate(flops=1000000, bytes_accessed=1000000, transcendentals=0),
    )(*(pltpu.with_memory_space_constraint(block, pltpu.VMEM) for block in blocks.values()), *rows)


def _step(size, grads, master, first, second):
    rows, width = master.shape
    f32 = jax.ShapeDtypeStruct((rows, width), jnp.float32)
    sums = _near_sums(grads, rows, width, size)
    parts = [sums[0], *_far_sums(sums, size)]

    devices = size * lax.axis_size("expert")
    kept = pltpu.VMEM((rows, width), jnp.float32)
    square = pltpu.VMEM((devices, 1, 128), jnp.float32)
    summed, square = _call(_finish_sum, (kept, square), *parts)
    squares = lax.all_to_all(square, ("expert", "dp"), 0, 0)
    state = (squares, summed, master, first, second)
    (own,) = _call(_weights, (pltpu.VMEM((rows, width), jnp.bfloat16),), *state)
    results = _call(_states, (f32,) * 4, *state)

    blocks = {0: own}
    for k in _outward(size):
        blocks[k * NEAR] = _swap(own, size, k * NEAR)
    for k in (0, *_outward(size)):
        blocks[k * NEAR + 2] = _swap(blocks[k * NEAR], size, 2)
    for offset in list(blocks):
        blocks[offset + 1] = _swap(blocks[offset], size, 1)
    placed = _placed(size, {k: block for k, block in blocks.items() if not k & 2})
    placed = _placed(size, {k: block for k, block in blocks.items() if k & 3 == 2}, placed)
    new_weights = _placed(size, {k: block for k, block in blocks.items() if k & 3 == 3}, placed)
    return results, new_weights


def shards(size, grads, master, first_moment, second_moment):
    results, new_weights = _step(size, grads[0, 0], master[0], first_moment[0], second_moment[0])
    new_weights = new_weights.reshape(1, -1, master.shape[2])
    return (*(result[None] for result in results), new_weights)


def solution(mesh):
    state = P("expert", "dp", None)
    size = mesh.shape["dp"]
    return jax.shard_map(
        functools.partial(shards, size),
        mesh=mesh,
        in_specs=(P("expert", "dp", None, None), state, state, state),
        out_specs=(state, state, state, state, P("expert", None, None)),
        check_vma=False,
    )
```

```python
import functools

import jax
import jax.numpy as jnp
from jax import lax
from jax.experimental import pallas as pl
from jax.experimental.pallas import tpu as pltpu
from jax.sharding import PartitionSpec as P

STEP = 10
NEAR = 4
VMEM = pl.BlockSpec(memory_space=pltpu.VMEM)


def _swap(array, size, offset):
    return lax.ppermute(array, "dp", [(i, i ^ offset) for i in range(size)])


def _call(body, outs, *args):
    return pl.pallas_call(
        body,
        out_shape=outs,
        in_specs=[VMEM] * len(args),
        out_specs=[VMEM] * len(outs),
        cost_estimate=pl.CostEstimate(flops=1000000, bytes_accessed=1000000, transcendentals=0),
    )(*(pltpu.with_memory_space_constraint(arg, pltpu.VMEM) for arg in args))


def _groups(size):
    far = size // NEAR
    return [[far - 1], [far - 2], list(reversed(range(1, far - 2))), [0]]


def _far_order(size):
    return [k for group in _groups(size) for k in group]


def _outward(size):
    far = size // NEAR
    return [3, 1, 2] if far == 4 else list(range(1, far))


def _copy_rows(wanted, blocks, *refs):
    *outs, done = refs
    me = lax.axis_index("dp")
    copies = []
    for offsets, out in zip(wanted, outs):
        for i, offset in enumerate(offsets):
            copies.append(pltpu.make_async_copy(blocks.at[me ^ offset], out.at[i], done.at[len(copies)]))
    for copy in copies:
        copy.start()
    for copy in copies:
        copy.wait()


def _cut(blocks, wanted):
    _, rows, width = blocks.shape
    return pl.pallas_call(
        functools.partial(_copy_rows, wanted),
        out_shape=[pltpu.VMEM((len(offsets), rows, width), blocks.dtype) for offsets in wanted],
        in_specs=[pl.BlockSpec(memory_space=pl.ANY)],
        out_specs=[VMEM] * len(wanted),
        scratch_shapes=[pltpu.SemaphoreType.DMA((sum(map(len, wanted)),))],
        cost_estimate=pl.CostEstimate(flops=1000000, bytes_accessed=1000000, transcendentals=0),
    )(pltpu.with_memory_space_constraint(blocks, pltpu.HBM))


def _near_sums(grads, rows, width, size):
    blocks = grads.reshape(size, rows, width)
    groups = _groups(size)
    order = _far_order(size)
    first = _cut(blocks, [[k * NEAR + j for k in groups[0]] for j in (2, 3)])
    wanted = [[k * NEAR + j for k in group] for group in groups[1:] for j in (2, 3)]
    rest = _cut(blocks, [[k * NEAR + j for k in order] for j in (0, 1)] + wanted)
    own, pair, *rest = rest
    rest = list(zip(rest[::2], rest[1::2]))
    moved = []
    for pieces in [first, *rest]:
        moved.append([_swap(pieces[0], size, 2), _swap(pieces[1], size, 3)])
    pair = _swap(pair, size, 1)
    sums = {}
    block = pltpu.VMEM((rows, width), jnp.float32)
    for g, group in enumerate(groups):
        at = [order.index(k) for k in group]
        totals = _call(functools.partial(_add_near, at), (block,) * len(at), own, pair, *moved[g])
        sums.update(zip(group, totals))
    return sums


def _add_near(at, own, pair, left, right, *totals):
    for i, (k, total) in enumerate(zip(at, totals)):
        here = own[k].astype(jnp.float32) + pair[k].astype(jnp.float32)
        total[...] = here + left[i].astype(jnp.float32) + right[i].astype(jnp.float32)


def _far_sums(sums, size):
    parts = []
    order = _far_order(size)[:-1]
    for k in order:
        parts.append(_swap(sums[k], size, k * NEAR))
    return parts


def _finish_sum(*refs):
    *parts, summed, square = refs
    total = parts[0][...]
    for part in parts[1:]:
        total = total + part[...]
    summed[...] = total
    own = jnp.sum(jnp.sum(total * total, axis=1, keepdims=True), axis=0, keepdims=True)
    square[...] = jnp.broadcast_to(own[None], square.shape)


def _update(squares, summed, master, first, second):
    norm = jnp.sqrt(jnp.sum(squares[...], axis=0))[:, :1]
    clip = 1.0 / jnp.maximum(norm, 1.0)
    clipped = clip * summed[...]
    new_first = 0.9 * first[...] + 0.1 * clipped
    new_second = 0.95 * second[...] + 0.05 * (clipped * clipped)
    first_fix = 1.0 - 0.9**STEP
    second_fix = 1.0 - 0.95**STEP
    direction = new_first / first_fix / (jnp.sqrt(new_second / second_fix) + 1e-08)
    new_master = master[...] - 0.001 * (direction + 0.1 * master[...])
    return new_master, new_first, new_second, direction


def _weights(squares, summed, master, first, second, own):
    own[...] = _update(squares, summed, master, first, second)[0].astype(jnp.bfloat16)


def _states(squares, summed, master, first, second, *outs):
    for out, value in zip(outs, _update(squares, summed, master, first, second)):
        out[...] = value


def _place(offsets, blocks, *refs):
    *_, out, done = refs
    me = lax.axis_index("dp")
    copies = [
        pltpu.make_async_copy(block, out.at[me ^ offset], done.at[i])
        for i, (offset, block) in enumerate(zip(offsets, blocks))
    ]
    for copy in copies:
        copy.start()
    for copy in copies:
        copy.wait()


def _placed(size, blocks, *rows):
    offsets = list(blocks)
    height, width = blocks[offsets[0]].shape

    def body(*refs):
        _place(offsets, refs[: len(offsets)], *refs[len(offsets) :])

    return pl.pallas_call(
        body,
        out_shape=jax.ShapeDtypeStruct((size, height, width), jnp.bfloat16),
        in_specs=[VMEM] * len(offsets) + [pl.BlockSpec(memory_space=pl.ANY)] * len(rows),
        out_specs=pl.BlockSpec(memory_space=pl.ANY),
        scratch_shapes=[pltpu.SemaphoreType.DMA((len(offsets),))],
        input_output_aliases={len(offsets): 0} if rows else {},
        cost_estimate=pl.CostEstimate(flops=1000000, bytes_accessed=1000000, transcendentals=0),
    )(*(pltpu.with_memory_space_constraint(block, pltpu.VMEM) for block in blocks.values()), *rows)


def _step(size, grads, master, first, second):
    rows, width = master.shape
    f32 = jax.ShapeDtypeStruct((rows, width), jnp.float32)
    sums = _near_sums(grads, rows, width, size)
    parts = [sums[0], *_far_sums(sums, size)]

    devices = size * lax.axis_size("expert")
    kept = pltpu.VMEM((rows, width), jnp.float32)
    square = pltpu.VMEM((devices, 1, 128), jnp.float32)
    summed, square = _call(_finish_sum, (kept, square), *parts)
    squares = lax.all_to_all(square, ("expert", "dp"), 0, 0)
    state = (squares, summed, master, first, second)
    (own,) = _call(_weights, (pltpu.VMEM((rows, width), jnp.bfloat16),), *state)
    results = _call(_states, (f32,) * 4, *state)

    blocks = {0: own}
    for k in _outward(size):
        blocks[k * NEAR] = _swap(own, size, k * NEAR)
    for k in (0, *_outward(size)):
        blocks[k * NEAR + 2] = _swap(blocks[k * NEAR], size, 2)
    for offset in list(blocks):
        blocks[offset + 1] = _swap(blocks[offset], size, 1)
    placed = _placed(size, {k: block for k, block in blocks.items() if not k & 2})
    placed = _placed(size, {k: block for k, block in blocks.items() if k & 3 == 2}, placed)
    new_weights = _placed(size, {k: block for k, block in blocks.items() if k & 3 == 3}, placed)
    return results, new_weights


def shards(size, grads, master, first_moment, second_moment):
    results, new_weights = _step(size, grads[0, 0], master[0], first_moment[0], second_moment[0])
    new_weights = new_weights.reshape(1, -1, master.shape[2])
    return (*(result[None] for result in results), new_weights)


def solution(mesh):
    state = P("expert", "dp", None)
    size = mesh.shape["dp"]
    return jax.shard_map(
        functools.partial(shards, size),
        mesh=mesh,
        in_specs=(P("expert", "dp", None, None), state, state, state),
        out_specs=(state, state, state, state, P("expert", None, None)),
        check_vma=False,
    )
```
